32 devices in a mesh: cells: 16 (over z, y, core), genes: 2 (over x).
Axes of the slice: x: 2, y: 2, z: 4, core: 2. Of those that a mesh axis runs over, the one named last changes fastest.
Arguments:
- counts: int32 [2048, 33280], P('cells', 'genes'), may hold values from 0 to 64, as said below
- live_rows: int32 [16], P('cells'), may hold values from 64 to 128, as said below
- left_basis: float32 [32, 2048], P(None, 'cells'), may hold values from -0.125 to 0.125
- right_basis: float32 [32, 33280], P(None, 'genes'), may hold values from -0.03125 to 0.03125
- right_start: float32 [16, 33280], P(None, 'genes'), may hold values from -0.03125 to 0.03125
Outputs:
- left_vectors: float32 [48, 2048], P(None, 'cells')
- right_vectors: float32 [48, 33280], P(None, 'genes')
- diag_blocks: float32 [3, 16, 16], replicated
- couple_blocks: float32 [3, 16, 16], replicated
The draws below stay inside these ranges and needn't reach their ends.
Inputs may be any that keep to these rules, and one draw needn't show every extreme that they name: `counts`: rows of a cell block at or beyond its live count are padding and are not part of the matrix. `live_rows`: entry b is the number of live rows, the first ones, of cell block b; some block is full in every draw.
All inputs are finite; a program needn't handle non-finite values.
Results may differ from the reference program's by a relative error of at most 0.0003.
Values sent between devices are 32-bit elements; how exact they have to be, the bound alone decides.
A program may use at most 64 MiB of HBM per device.

```python
import jax
import jax.numpy as jnp
from jax import lax

CELL_DEV = 128
GENES = 33280
BASIS = 32
BLOCK = 16
STEPS = 3
CELL_BLOCKS = 16
CELLS = 2048


def draw_counts(key, part):
    first = jax.random.fold_in(key, 11)
    second = jax.random.fold_in(key, 12)
    third = jax.random.fold_in(key, 13)
    powers = jax.random.randint(first, (1, GENES), 0, 7)
    ceiling = jnp.left_shift(jnp.ones((1, GENES), jnp.int32), powers)
    values = jax.random.randint(second, (CELLS, GENES), 0, ceiling + 1)
    present = jax.random.randint(third, (CELLS, GENES), 0, 5) < 2
    return jnp.where(present, values, 0).astype(jnp.int32)


def draw_live_rows(key, part):
    first = jax.random.fold_in(key, 21)
    second = jax.random.fold_in(key, 22)
    lengths = jax.random.randint(first, (CELL_BLOCKS,), CELL_DEV // 2, CELL_DEV + 1)
    chosen = jax.random.randint(second, (), 0, CELL_BLOCKS)
    places = jnp.arange(CELL_BLOCKS, dtype=jnp.int32)
    return jnp.where(places == chosen, CELL_DEV, lengths).astype(jnp.int32)


def shard_levels(rng, shape, pieces, least, largest):
    def one(axis_at, parts):
        draws = jax.random.uniform(jax.random.fold_in(jax.random.fold_in(rng, 6), axis_at), (parts,), jnp.float32, least / len(pieces), largest / len(pieces))
        return jnp.repeat(jnp.exp(draws), shape[axis_at] // parts).reshape((-1,) + (1,) * (len(shape) - axis_at - 1))

    loudness = one(*pieces[0])
    for cut in pieces[1:]:
        loudness = loudness * one(*cut)
    return loudness


def centred(rng, shape, scale, reach, shards=(), kind=jnp.bfloat16):
    loudness = shard_levels(rng, shape, shards, -0.22, 0.18) if shards else 1.0
    drawn = jax.random.normal(rng, shape, jnp.float32) * scale * loudness
    return jnp.minimum(jnp.maximum(drawn, -reach), reach).astype(kind)


def setup_inputs(seed: int = 0) -> dict:
    keys = jax.random.split(jax.random.key(seed), 6)
    counts = draw_counts(jax.random.fold_in(keys[5], 71), 0)
    live_rows = draw_live_rows(jax.random.fold_in(keys[5], 71), 0)
    left_basis = centred(keys[2], (BASIS, CELLS), CELLS ** -0.5, 0.125, ((1, 16),), jnp.float32)
    right_basis = centred(keys[3], (BASIS, GENES), GENES ** -0.5, 0.03125, ((1, 2),), jnp.float32)
    right_start = centred(keys[4], (BLOCK, GENES), GENES ** -0.5, 0.03125, ((1, 2),), jnp.float32)
    return {"counts": counts, "live_rows": live_rows, "left_basis": left_basis, "right_basis": right_basis, "right_start": right_start}


HIGHEST = lax.Precision.HIGHEST

def matmul(lhs, rhs):
    return jnp.dot(lhs.astype(jnp.float32), rhs.astype(jnp.float32), precision=HIGHEST, preferred_element_type=jnp.float32)

def outer_rows(lhs, rhs):
    return lax.dot_general(lhs.astype(jnp.float32), rhs.astype(jnp.float32), (((1,), (1,)), ((), ())), precision=HIGHEST, preferred_element_type=jnp.float32)

def orthonormal_block(vectors, spanning):
    coeffs = outer_rows(vectors, spanning)
    cleaned = vectors - matmul(coeffs, spanning)
    coeffs = outer_rows(cleaned, spanning)
    cleaned = cleaned - matmul(coeffs, spanning)
    squares = outer_rows(cleaned, cleaned)
    factor = jnp.linalg.cholesky(squares)
    result = lax.linalg.triangular_solve(factor, cleaned, left_side=True, lower=True)
    return (result, factor)

def reference(counts, live_rows, left_basis, right_basis, right_start):
    within = jnp.arange(CELL_DEV, dtype=jnp.int32)[None, :] < live_rows[:, None]
    weights = within.reshape(CELLS).astype(jnp.float32)
    logged = jnp.where(weights[:, None] > 0, jnp.log1p(counts.astype(jnp.float32)), 0.0)
    live_total = jnp.sum(live_rows).astype(jnp.float32)
    column_mean = lax.optimization_barrier(jnp.sum(logged, axis=0)) / live_total
    factor_scale = lax.rsqrt(live_total)
    slots_left = jnp.concatenate([left_basis * weights[None, :], jnp.zeros((STEPS * BLOCK, CELLS), jnp.float32)], axis=0)
    slots_right = jnp.concatenate([right_basis, right_start, jnp.zeros(((STEPS - 1) * BLOCK, GENES), jnp.float32)], axis=0)
    current = right_start
    left_blocks, right_blocks, diag_list, couple_list = ([], [], [], [])
    for iteration in range(STEPS):
        projected = (outer_rows(current, logged) - matmul(current, column_mean)[:, None] * weights[None, :]) * factor_scale
        leftvec, diag_factor = orthonormal_block(projected, slots_left)
        position = BASIS + iteration * BLOCK
        slots_left = slots_left.at[position:position + BLOCK].set(leftvec)
        projected = (matmul(leftvec, logged) - lax.optimization_barrier(jnp.sum(leftvec, axis=1))[:, None] * column_mean[None, :]) * factor_scale
        current, side_factor = orthonormal_block(projected, slots_right)
        if iteration + 1 < STEPS:
            slots_right = slots_right.at[position + BLOCK:position + 2 * BLOCK].set(current)
        left_blocks.append(leftvec)
        right_blocks.append(current)
        diag_list.append(diag_factor)
        couple_list.append(side_factor)
    left_vectors = jnp.concatenate(left_blocks, axis=0) * jnp.sqrt(jnp.float32(CELLS))
    right_vectors = jnp.concatenate(right_blocks, axis=0) * jnp.sqrt(jnp.float32(GENES))
    return (left_vectors, right_vectors, jnp.stack(diag_list), jnp.stack(couple_list))
```

```python
import functools
import math

import jax
import jax.numpy as jnp
from jax import lax
from jax.experimental import pallas as pl
from jax.experimental.pallas import tpu as pltpu
from jax.sharding import PartitionSpec as P

BASIS = 32
BLOCK = 16
STEPS = 3
SLOTS = BASIS + STEPS * BLOCK
LANES = 128
F32 = jnp.float32
BF16 = jnp.bfloat16
HIGHEST = lax.Precision.HIGHEST
MESH = pl.DeviceIdType.MESH


def exact(lhs, rhs):
    return jnp.dot(lhs, rhs, precision=HIGHEST, preferred_element_type=F32)


def exact_rows(lhs, rhs):
    return lax.dot_general(
        lhs, rhs, (((1,), (1,)), ((), ())), precision=HIGHEST, preferred_element_type=F32
    )


def split(values):
    high = values.astype(BF16)
    return high, (values - high.astype(F32)).astype(BF16)


def product(high, both, rhs_high, rhs_low, dims):
    rows = high.shape[0]
    first = lax.dot_general(both, rhs_high, (dims, ((), ())), preferred_element_type=F32)
    second = lax.dot_general(high, rhs_low, (dims, ((), ())), preferred_element_type=F32)
    return first[:rows] + (first[rows:] + second)


ALONG = ((1,), (0,))
ROWS = ((1,), (1,))


def loop(start, stop, step):
    def one(k, carry):
        step(k)
        return carry

    lax.fori_loop(start, stop, one, 0)


def orthonormal(gram, near, lower, spanning, vectors):
    lane = lax.broadcasted_iota(jnp.int32, (BLOCK, LANES), 1)
    row = lax.broadcasted_iota(jnp.int32, (BLOCK, LANES), 0)
    coeffs = jnp.where(lane < SLOTS, gram, 0.0)
    squares = gram[:, SLOTS : SLOTS + BLOCK]
    combined = coeffs + coeffs - (exact(coeffs, near) + exact_rows(coeffs, lower))
    residue = coeffs - (exact(combined, near) + exact_rows(combined, lower))
    squares = squares - exact_rows(combined, coeffs) - exact_rows(residue, combined)
    cleaned = vectors - exact(combined, spanning)
    change = jnp.where(lane == row + SLOTS, 1.0, -combined)
    parts = [squares, cleaned, residue, change]
    for k in range(BLOCK):
        pivot = parts[0][k : k + 1, k : k + 1]
        root = lax.rsqrt(pivot)
        root = root * (1.5 - 0.5 * pivot * root * root)
        column = parts[0][:, k : k + 1] * root
        after = []
        for part in parts:
            scaled = part[k : k + 1, :] * root
            places = lax.broadcasted_iota(jnp.int32, part.shape, 0)
            after.append(
                jnp.where(places > k, part - column * scaled, jnp.where(places == k, scaled, part))
            )
        parts = after
    spot = lax.broadcasted_iota(jnp.int32, (BLOCK, BLOCK), 0)
    other = lax.broadcasted_iota(jnp.int32, (BLOCK, BLOCK), 1)
    upper = jnp.where(other >= spot, parts[0], 0.0)
    factor = exact_rows(jnp.where(other == spot, 1.0, 0.0).astype(F32), upper)
    return parts[1], factor, parts[2], parts[3]


def kernel(
    n, g, width, scales,
    live, counts, left_basis, right_basis, right_start,
    left_out, right_out, diag_out, couple_out,
    cnt, logged, bhi, blo, rb, sl, mr, el, tl, er, tr,
    w, ra, rt, pb, w8, ra8, rt8, pb8, gram0, gram, xg0, xg,
    in_sem, as_sem, ar_sem, bs_sem, br_sem, cs_sem, cr_sem, ds_sem,
    g0s_sem, g0r_sem, gs_sem, gr_sem, x0s_sem, x0r_sem, xs_sem, xr_sem,
):
    cells, genes = counts.shape
    me = lax.axis_index("cells")
    mine = lax.axis_index("genes")
    core = lax.rem(me, 2)
    chip = me // 2
    h = n // 2
    sibling = me + 1 - 2 * core

    def along_cells(src, dst, send, recv, peer):
        return pltpu.make_async_remote_copy(
            src_ref=src, dst_ref=dst, send_sem=send, recv_sem=recv,
            device_id=(peer, mine), device_id_type=MESH,
        )

    def along_genes(src, dst, send, recv, peer):
        return pltpu.make_async_remote_copy(
            src_ref=src, dst_ref=dst, send_sem=send, recv_sem=recv,
            device_id=(me, peer), device_id_type=MESH,
        )

    loads = []
    for d in range(n):
        cols = max(0, min(width, genes - d * width))
        if cols:
            here = pl.ds(d * width, cols)
            loads.append((d, [
                pltpu.make_async_copy(counts.at[:, here], cnt.at[d, :, pl.ds(0, cols)], in_sem.at[d, 0]),
                pltpu.make_async_copy(right_basis.at[:, here], rb.at[d, pl.ds(0, BASIS), pl.ds(0, cols)], in_sem.at[d, 1]),
                pltpu.make_async_copy(right_start.at[:, here], rb.at[d, pl.ds(BASIS, BLOCK), pl.ds(0, cols)], in_sem.at[d, 2]),
            ]))
        if cols < width:
            cnt[d, :, cols:] = jnp.zeros((cells, width - cols), jnp.int32)
            rb[d, :, cols:] = jnp.zeros((BASIS + BLOCK, width - cols), F32)
    for _, trio in loads:
        trio[0].start()
    for _, trio in loads:
        trio[1].start()
        trio[2].start()

    barrier = pltpu.get_barrier_semaphore()

    def greet_cells(k):
        pl.semaphore_signal(barrier, inc=1, device_id=(lax.rem(me + k, n), mine), device_id_type=MESH)

    def greet_genes(k):
        pl.semaphore_signal(barrier, inc=1, device_id=(me, lax.rem(mine + k, g)), device_id_type=MESH)

    loop(1, n, greet_cells)
    loop(1, g, greet_genes)
    pl.semaphore_wait(barrier, n - 1 + g - 1)

    def spread(copy, buf, at, size, send, recv):
        def go(k):
            copy(buf.at[at], buf.at[at], send.at[k], recv.at[at], lax.rem(at + k, size)).start()

        loop(1, size, go)

    def gathered(copy, buf, at, size, send, recv):
        def end(k):
            source = lax.rem(at + size - k, size)
            item = copy(buf.at[source], buf.at[source], send.at[k], recv.at[source], lax.rem(at + k, size))
            item.wait_send()
            item.wait_recv()

        loop(1, size, end)
        return lax.fori_loop(
            1, size, lambda k, total: total + buf[k], buf[0]
        )

    def reduce_scatter(produce, part, fromcore, fromchips, result):
        def first(k):
            t = lax.rem(chip + 1 + k, h)
            d = 2 * t + 1 - core
            produce(d)
            along_cells(part.at[d], fromcore.at[t], as_sem.at[t], ar_sem.at[t], sibling).start()

        loop(0, h, first)

        def join(t):
            d = 2 * t + core
            produce(d)
            along_cells(part.at[d], fromcore.at[t], as_sem.at[t], ar_sem.at[t], sibling).wait_recv()
            part[d] = part[d] + fromcore[t]
            return d

        def second(k):
            t = lax.rem(chip + 1 + k, h)
            d = join(t)
            along_cells(part.at[d], fromchips.at[chip], bs_sem.at[t], br_sem.at[chip], d).start()

        loop(0, h - 1, second)
        join(chip)
        result[me] = part[me]

        def third(k):
            t = lax.rem(chip + h - k, h)
            along_cells(part.at[me], fromchips.at[t], bs_sem.at[t], br_sem.at[t], sibling).wait_recv()
            result[me] = result[me] + fromchips[t]

        loop(1, h, third)

    def all_gather(part, fromcore, fromchips, result, consume):
        def go(k):
            t = lax.rem(chip + k, h)
            along_cells(result.at[me], result.at[me], cs_sem.at[t], cr_sem.at[me], 2 * t + core).start()

        loop(1, h, go)
        along_cells(result.at[me], result.at[me], ds_sem.at[chip], cr_sem.at[me], sibling).start()
        consume(me)

        def pass_on(k):
            t = lax.rem(chip + h - k, h)
            d = 2 * t + core
            along_cells(result.at[d], result.at[d], cs_sem.at[t], cr_sem.at[d], sibling).wait_recv()
            along_cells(result.at[d], result.at[d], ds_sem.at[t], cr_sem.at[d], sibling).start()
            consume(d)

        loop(1, h, pass_on)

        def rest(k):
            t = lax.rem(chip + h - k, h)
            d = 2 * t + 1 - core
            along_cells(result.at[d], result.at[d], cs_sem.at[t], cr_sem.at[d], sibling).wait_recv()
            consume(d)

        loop(0, h, rest)

        def ended(t):
            along_cells(part.at[t], fromcore.at[t], as_sem.at[t], ar_sem.at[t], sibling).wait_send()
            along_cells(result.at[t], result.at[t], ds_sem.at[t], cr_sem.at[t], sibling).wait_send()

        loop(0, h, ended)

        def ended_chips(k):
            t = lax.rem(chip + k, h)
            along_cells(part.at[t], fromchips.at[t], bs_sem.at[t], br_sem.at[t], sibling).wait_send()
            along_cells(result.at[t], result.at[t], cs_sem.at[t], cr_sem.at[t], sibling).wait_send()

        loop(1, h, ended_chips)

    live_here = live[0]
    weights_row = jnp.where(
        lax.broadcasted_iota(jnp.int32, (1, cells), 1) < live_here, 1.0, 0.0
    ).astype(F32)
    weights = jnp.where(
        lax.broadcasted_iota(jnp.int32, (cells, LANES), 0) < live_here, 1.0, 0.0
    ).astype(F32)
    for table in (sl, mr, tl, tr):
        table[...] = jnp.zeros_like(table)
    same = jnp.where(
        lax.broadcasted_iota(jnp.int32, (LANES, LANES), 0)
        == lax.broadcasted_iota(jnp.int32, (LANES, LANES), 1),
        1.0, 0.0,
    ).astype(F32)
    el[...] = same
    er[...] = same
    sl[0:BASIS] = left_basis[...] * weights_row
    gram0[me] = exact_rows(sl[0:BASIS], sl[...])
    spread(along_cells, gram0, me, n, g0s_sem, g0r_sem)

    for _, trio in loads:
        trio[0].wait()
    tiles = width // LANES

    def take_log(d):
        for i in range(tiles):
            here = slice(i * LANES, (i + 1) * LANES)
            values = jnp.log(1.0 + cnt[d, :, here].astype(F32)) * weights
            logged[d, :, here] = values
            w8[d, :, here] = jnp.sum(values.reshape(cells // 8, 8, LANES), axis=0)

    loop(0, n, take_log)
    total_at, total_lane = genes // width, genes % width
    w8[total_at, :, total_lane : total_lane + LANES] = jnp.where(
        lax.broadcasted_iota(jnp.int32, (8, LANES), 0) == 0, live_here.astype(F32), 0.0
    )

    reduce_scatter(lambda d: None, w8, ra8, rt8, pb8)
    for _, trio in loads:
        trio[1].wait()
        trio[2].wait()

    def fill(d):
        high, low = split(rb[d])
        bhi[d, cells : cells + BASIS + BLOCK] = high
        blo[d, cells : cells + BASIS + BLOCK] = low
        blank = jnp.zeros((LANES - BASIS - BLOCK, width), BF16)
        bhi[d, cells + BASIS + BLOCK :] = blank
        blo[d, cells + BASIS + BLOCK :] = blank

    loop(0, n, fill)
    all_gather(w8, ra8, rt8, pb8, lambda d: None)
    live_total = jnp.sum(
        pb8[total_at, :, total_lane : total_lane + LANES], axis=0, keepdims=True
    )
    inverse = 1.0 / live_total
    factor_scale = lax.rsqrt(live_total)
    factor_scale = factor_scale * (1.5 - 0.5 * live_total * factor_scale * factor_scale)

    xg0[mine] = jnp.zeros((BASIS + BLOCK, 2 * LANES), F32)

    def center(d):
        for i in range(tiles):
            here = slice(i * LANES, (i + 1) * LANES)
            mean = jnp.sum(pb8[d, :, here], axis=0, keepdims=True) * inverse
            mean = jnp.where(d * width + i * LANES < genes, mean, 0.0)
            high, low = split((logged[d, :, here] - weights * mean) * factor_scale)
            bhi[d, 0:cells, here] = high
            blo[d, 0:cells, here] = low
        high, low = split(rb[d])
        both = jnp.concatenate([high, low], axis=0)
        xg0[mine] = xg0[mine] + product(high, both, bhi[d], blo[d], ROWS)

    loop(0, n, center)
    spread(along_genes, xg0, mine, g, x0s_sem, x0r_sem)
    el[0:BASIS] = gathered(along_cells, gram0, me, n, g0s_sem, g0r_sem)
    el[...] = jnp.where((same > 0) & (lax.broadcasted_iota(jnp.int32, (LANES, LANES), 0) >= BASIS), 1.0, el[...])
    cross = gathered(along_genes, xg0, mine, g, x0s_sem, x0r_sem)
    mr[0 : BASIS + BLOCK] = cross[:, :cells]
    er[0 : BASIS + BLOCK] = cross[:, cells:]
    whole = genes // width

    def step(j):
        position = pl.multiple_of(BASIS + j * BLOCK, BLOCK)
        vectors = mr[pl.ds(position, BLOCK)]
        sl[SLOTS : SLOTS + BLOCK] = vectors
        gram[me] = exact_rows(vectors, sl[...])
        spread(along_cells, gram, me, n, gs_sem, gr_sem)
        total = gathered(along_cells, gram, me, n, gs_sem, gr_sem)
        leftvec, factor, against, _ = orthonormal(total, el[...], tl[...], sl[...], vectors)
        diag_out[j] = factor
        sl[pl.ds(position, BLOCK)] = leftvec
        el[pl.ds(position, BLOCK)] = el[pl.ds(position, BLOCK)] + against
        tl[pl.ds(position, BLOCK)] = against
        left_out[pl.ds(position - BASIS, BLOCK)] = leftvec * scales[0]
        high, low = split(leftvec)
        both = jnp.concatenate([high, low], axis=0)

        def produce(d):
            w[d] = product(high, both, bhi[d, 0:cells], blo[d, 0:cells], ALONG)

        reduce_scatter(produce, w, ra, rt, pb)
        xg[j, mine] = jnp.zeros((BLOCK, 2 * LANES), F32)

        def consume(d):
            phigh, plow = split(pb[d])
            bhi[d, cells + SLOTS : cells + SLOTS + BLOCK] = phigh
            blo[d, cells + SLOTS : cells + SLOTS + BLOCK] = plow
            pboth = jnp.concatenate([phigh, plow], axis=0)
            xg[j, mine] = xg[j, mine] + product(phigh, pboth, bhi[d], blo[d], ROWS)

        all_gather(w, ra, rt, pb, consume)
        box = xg.at[j]
        spread(along_genes, box, mine, g, xs_sem.at[j], xr_sem.at[j])
        total = gathered(along_genes, box, mine, g, xs_sem.at[j], xr_sem.at[j])
        projected, factor, against, change = orthonormal(
            total[:, cells:], er[...], tr[...], mr[...], total[:, :cells]
        )
        couple_out[j] = factor
        later = pl.multiple_of(position + BLOCK, BLOCK)
        mr[pl.ds(later, BLOCK)] = projected
        er[pl.ds(later, BLOCK)] = er[pl.ds(later, BLOCK)] + against
        tr[pl.ds(later, BLOCK)] = against
        chigh, clow = split(change)
        cboth = jnp.concatenate([chigh, clow], axis=0)

        def right(d):
            fresh = product(chigh, cboth, bhi[d, cells:], blo[d, cells:], ALONG)
            vhigh, vlow = split(fresh)
            bhi[d, pl.ds(cells + later, BLOCK)] = vhigh
            blo[d, pl.ds(cells + later, BLOCK)] = vlow
            return fresh * scales[1]

        rows = pl.ds(position - BASIS, BLOCK)

        def emit(d):
            right_out[rows, pl.ds(pl.multiple_of(d * width, LANES), width)] = right(d)

        loop(0, whole, emit)
        if genes % width:
            right_out[rows, whole * width : genes] = right(whole)[:, : genes % width]

    loop(0, STEPS, step)


def body(counts, live_rows, left_basis, right_basis, right_start):
    cells, genes = counts.shape
    n = lax.axis_size("cells")
    g = lax.axis_size("genes")
    h = n // 2
    width = -(-(genes // LANES + 1) // n) * LANES
    scales = (math.sqrt(float(cells * n)), math.sqrt(float(genes * g)))
    vmem = pl.BlockSpec(memory_space=pltpu.VMEM)
    anywhere = pl.BlockSpec(memory_space=pl.ANY)
    square = pltpu.VMEM((LANES, LANES), F32)
    dma = lambda *shape: pltpu.SemaphoreType.DMA(shape)
    out_shape = (
        jax.ShapeDtypeStruct((STEPS * BLOCK, cells), F32),
        jax.ShapeDtypeStruct((STEPS * BLOCK, genes), F32),
        jax.ShapeDtypeStruct((STEPS, BLOCK, BLOCK), F32),
        jax.ShapeDtypeStruct((STEPS, BLOCK, BLOCK), F32),
    )
    buffers = lambda rows: [
        pltpu.VMEM((n, rows, width), F32),
        pltpu.VMEM((h, rows, width), F32),
        pltpu.VMEM((h, rows, width), F32),
        pltpu.VMEM((n, rows, width), F32),
    ]
    scratch = [
        pltpu.VMEM((n, cells, width), jnp.int32),
        pltpu.VMEM((n, cells, width), F32),
        pltpu.VMEM((n, cells + LANES, width), BF16),
        pltpu.VMEM((n, cells + LANES, width), BF16),
        pltpu.VMEM((n, BASIS + BLOCK, width), F32),
        square, square, square, square, square, square,
        *buffers(BLOCK),
        *buffers(8),
        pltpu.VMEM((n, BASIS, LANES), F32),
        pltpu.VMEM((n, BLOCK, LANES), F32),
        pltpu.VMEM((g, BASIS + BLOCK, 2 * LANES), F32),
        pltpu.VMEM((STEPS, g, BLOCK, 2 * LANES), F32),
        dma(n, 3),
        dma(h), dma(h), dma(h), dma(h), dma(h), dma(n), dma(h),
        dma(n), dma(n), dma(n), dma(n),
        dma(g), dma(g), dma(STEPS, g), dma(STEPS, g),
    ]
    return pl.pallas_call(
        functools.partial(kernel, n, g, width, scales),
        out_shape=out_shape,
        in_specs=[pl.BlockSpec(memory_space=pltpu.SMEM), anywhere, vmem, anywhere, anywhere],
        out_specs=(vmem, vmem, vmem, vmem),
        scratch_shapes=scratch,
        compiler_params=pltpu.CompilerParams(
            collective_id=0, has_side_effects=True, vmem_limit_bytes=66 * 1000 * 1000
        ),
    )(live_rows, counts, left_basis, right_basis, right_start)


def solution(mesh):
    in_specs = (
        P("cells", "genes"),
        P("cells"),
        P(None, "cells"),
        P(None, "genes"),
        P(None, "genes"),
    )
    out_specs = (P(None, "cells"), P(None, "genes"), P(), P())
    return jax.shard_map(body, mesh=mesh, in_specs=in_specs, out_specs=out_specs, check_vma=False)
```

```python
import functools
import math

import jax
import jax.numpy as jnp
from jax import lax
from jax.experimental import pallas as pl
from jax.experimental.pallas import tpu as pltpu
from jax.sharding import PartitionSpec as P

BASIS = 32
BLOCK = 16
STEPS = 3
SLOTS = BASIS + STEPS * BLOCK
LANES = 128
F32 = jnp.float32
BF16 = jnp.bfloat16
HIGHEST = lax.Precision.HIGHEST
MESH = pl.DeviceIdType.MESH


def exact(lhs, rhs):
    return jnp.dot(lhs, rhs, precision=HIGHEST, preferred_element_type=F32)


def exact_rows(lhs, rhs):
    return lax.dot_general(
        lhs, rhs, (((1,), (1,)), ((), ())), precision=HIGHEST, preferred_element_type=F32
    )


def split(values):
    high = values.astype(BF16)
    return high, (values - high.astype(F32)).astype(BF16)


def product(high, both, rhs_high, rhs_low, dims):
    rows = high.shape[0]
    first = lax.dot_general(both, rhs_high, (dims, ((), ())), preferred_element_type=F32)
    second = lax.dot_general(high, rhs_low, (dims, ((), ())), preferred_element_type=F32)
    return first[:rows] + (first[rows:] + second)


ALONG = ((1,), (0,))
ROWS = ((1,), (1,))


def loop(start, stop, step):
    def one(k, carry):
        step(k)
        return carry

    lax.fori_loop(start, stop, one, 0)


def orthonormal(gram, near, lower, spanning, vectors):
    lane = lax.broadcasted_iota(jnp.int32, (BLOCK, LANES), 1)
    row = lax.broadcasted_iota(jnp.int32, (BLOCK, LANES), 0)
    coeffs = jnp.where(lane < SLOTS, gram, 0.0)
    squares = gram[:, SLOTS : SLOTS + BLOCK]
    combined = coeffs + coeffs - (exact(coeffs, near) + exact_rows(coeffs, lower))
    residue = coeffs - (exact(combined, near) + exact_rows(combined, lower))
    squares = squares - exact_rows(combined, coeffs) - exact_rows(residue, combined)
    cleaned = vectors - exact(combined, spanning)
    change = jnp.where(lane == row + SLOTS, 1.0, -combined)
    parts = [squares, cleaned, residue, change]
    for k in range(BLOCK):
        pivot = parts[0][k : k + 1, k : k + 1]
        root = lax.rsqrt(pivot)
        root = root * (1.5 - 0.5 * pivot * root * root)
        column = parts[0][:, k : k + 1] * root
        after = []
        for part in parts:
            scaled = part[k : k + 1, :] * root
            places = lax.broadcasted_iota(jnp.int32, part.shape, 0)
            after.append(
                jnp.where(places > k, part - column * scaled, jnp.where(places == k, scaled, part))
            )
        parts = after
    spot = lax.broadcasted_iota(jnp.int32, (BLOCK, BLOCK), 0)
    other = lax.broadcasted_iota(jnp.int32, (BLOCK, BLOCK), 1)
    upper = jnp.where(other >= spot, parts[0], 0.0)
    factor = exact_rows(jnp.where(other == spot, 1.0, 0.0).astype(F32), upper)
    return parts[1], factor, parts[2], parts[3]


def kernel(
    n, g, width, scales,
    live, counts, left_basis, right_basis, right_start,
    left_out, right_out, diag_out, couple_out,
    cnt, logged, bhi, blo, rb, sl, mr, el, tl, er, tr,
    w, ra, rt, rz, pb, w8, ra8, rt8, rz8, pb8, chg, gram0, gram, xg0, xg,
    in_sem, as_sem, ar_sem, bs_sem, br_sem, cs_sem, cr_sem, ds_sem, fs_sem, zs_sem, zr_sem,
    g0s_sem, g0r_sem, gs_sem, gr_sem, x0s_sem, x0r_sem, xs_sem, xr_sem,
):
    cells, genes = counts.shape
    me = lax.axis_index("cells")
    mine = lax.axis_index("genes")
    core = lax.rem(me, 2)
    chip = me // 2
    h = n // 2
    b = 1 << ((h.bit_length() - 1) // 2)
    b = b if h % b == 0 else 1
    a = h // b
    zi, yi = chip // b, lax.rem(chip, b)
    sibling = me + 1 - 2 * core

    def along_cells(src, dst, send, recv, peer):
        return pltpu.make_async_remote_copy(
            src_ref=src, dst_ref=dst, send_sem=send, recv_sem=recv,
            device_id=(peer, mine), device_id_type=MESH,
        )

    def along_genes(src, dst, send, recv, peer):
        return pltpu.make_async_remote_copy(
            src_ref=src, dst_ref=dst, send_sem=send, recv_sem=recv,
            device_id=(me, peer), device_id_type=MESH,
        )

    loads = []
    for d in range(n):
        cols = max(0, min(width, genes - d * width))
        if cols:
            here = pl.ds(d * width, cols)
            loads.append((d, [
                pltpu.make_async_copy(counts.at[:, here], cnt.at[d, :, pl.ds(0, cols)], in_sem.at[d, 0]),
                pltpu.make_async_copy(right_basis.at[:, here], rb.at[d, pl.ds(0, BASIS), pl.ds(0, cols)], in_sem.at[d, 1]),
                pltpu.make_async_copy(right_start.at[:, here], rb.at[d, pl.ds(BASIS, BLOCK), pl.ds(0, cols)], in_sem.at[d, 2]),
            ]))
        if cols < width:
            cnt[d, :, cols:] = jnp.zeros((cells, width - cols), jnp.int32)
            rb[d, :, cols:] = jnp.zeros((BASIS + BLOCK, width - cols), F32)
    for _, trio in loads:
        trio[0].start()
    for _, trio in loads:
        trio[1].start()
        trio[2].start()

    barrier = pltpu.get_barrier_semaphore()

    def greet_cells(k):
        pl.semaphore_signal(barrier, inc=1, device_id=(lax.rem(me + k, n), mine), device_id_type=MESH)

    def greet_genes(k):
        pl.semaphore_signal(barrier, inc=1, device_id=(me, lax.rem(mine + k, g)), device_id_type=MESH)

    loop(1, n, greet_cells)
    loop(1, g, greet_genes)
    pl.semaphore_wait(barrier, n - 1 + g - 1)

    def spread(copy, buf, at, size, send, recv):
        def go(k):
            copy(buf.at[at], buf.at[at], send.at[k], recv.at[at], lax.rem(at + k, size)).start()

        loop(1, size, go)

    def gathered(copy, buf, at, size, send, recv):
        def end(k):
            source = lax.rem(at + size - k, size)
            item = copy(buf.at[source], buf.at[source], send.at[k], recv.at[source], lax.rem(at + k, size))
            item.wait_send()
            item.wait_recv()

        loop(1, size, end)
        return lax.fori_loop(
            1, size, lambda k, total: total + buf[k], buf[0]
        )

    def order(k):
        return lax.rem(zi + 1 + lax.rem(k, a), a), lax.rem(yi + 1 + k // a, b)

    def reduce_scatter(produce, part, fromcore, fromy, fromz, result):
        def first(k):
            z, y = order(k)
            t = z * b + y
            d = 2 * t + 1 - core
            produce(d)
            along_cells(part.at[d], fromcore.at[t], as_sem.at[t], ar_sem.at[t], sibling).start()

        loop(0, h, first)

        def join(t):
            d = 2 * t + core
            produce(d)
            along_cells(part.at[d], fromcore.at[t], as_sem.at[t], ar_sem.at[t], sibling).wait_recv()
            part[d] = part[d] + fromcore[t]
            return d

        def second(k):
            z, y = order(k)
            t = z * b + y
            d = join(t)
            to = z * b + yi
            along_cells(part.at[d], fromy.at[to], bs_sem.at[t], br_sem.at[to], 2 * (zi * b + y) + core).start()

        loop(0, h - a, second)

        def complete(z):
            d = join(z * b + yi)

            def add(k):
                source = z * b + lax.rem(yi + k, b)
                along_cells(part.at[d], fromy.at[source], bs_sem.at[source], br_sem.at[source], sibling).wait_recv()
                part[d] = part[d] + fromy[source]

            loop(1, b, add)
            return d

        def third(k):
            z = lax.rem(zi + k, a)
            d = complete(z)
            along_cells(part.at[d], fromz.at[zi], zs_sem.at[z], zr_sem.at[zi], d).start()

        loop(1, a, third)
        complete(zi)
        result[me] = part[me]

        def fourth(k):
            z = lax.rem(zi + a - k, a)
            along_cells(part.at[me], fromz.at[z], zs_sem.at[z], zr_sem.at[z], sibling).wait_recv()
            result[me] = result[me] + fromz[z]

        loop(1, a, fourth)

    def all_gather(part, fromcore, fromy, fromz, result, consume):
        def relay(z):
            t = z * b + yi
            d = 2 * t + core

            def to_y(k):
                y = lax.rem(yi + k, b)
                along_cells(result.at[d], result.at[d], fs_sem.at[z * b + y], cr_sem.at[d], 2 * (zi * b + y) + core).start()

            loop(1, b, to_y)
            along_cells(result.at[d], result.at[d], ds_sem.at[t], cr_sem.at[d], sibling).start()

        def arrived(d):
            along_cells(result.at[d], result.at[d], ds_sem.at[0], cr_sem.at[d], sibling).wait_recv()

        def go(k):
            z = lax.rem(zi + k, a)
            along_cells(result.at[me], result.at[me], cs_sem.at[z], cr_sem.at[me], 2 * (z * b + yi) + core).start()

        loop(1, a, go)
        relay(zi)
        consume(me)

        def pass_z(k):
            z = lax.rem(zi + a - k, a)
            d = 2 * (z * b + yi) + core
            arrived(d)
            relay(z)
            consume(d)

        loop(1, a, pass_z)

        def pass_y(k):
            z = lax.rem(zi + a - lax.rem(k, a), a)
            t = z * b + lax.rem(yi + 1 + k // a, b)
            d = 2 * t + core
            arrived(d)
            along_cells(result.at[d], result.at[d], ds_sem.at[t], cr_sem.at[d], sibling).start()
            consume(d)

        loop(0, h - a, pass_y)

        def rest(k):
            z = lax.rem(zi + a - lax.rem(k, a), a)
            t = z * b + lax.rem(yi + k // a, b)
            d = 2 * t + 1 - core
            arrived(d)
            consume(d)

        loop(0, h, rest)

        def ended(t):
            along_cells(part.at[t], fromcore.at[t], as_sem.at[t], ar_sem.at[t], sibling).wait_send()
            along_cells(result.at[t], result.at[t], ds_sem.at[t], cr_sem.at[t], sibling).wait_send()

        loop(0, h, ended)

        def ended_y(k):
            z, y = order(k)
            t = z * b + y
            along_cells(part.at[t], fromy.at[t], bs_sem.at[t], br_sem.at[t], sibling).wait_send()
            along_cells(result.at[t], result.at[t], fs_sem.at[t], cr_sem.at[t], sibling).wait_send()

        loop(0, h - a, ended_y)

        def ended_z(k):
            z = lax.rem(zi + k, a)
            along_cells(part.at[z], fromz.at[z], zs_sem.at[z], zr_sem.at[z], sibling).wait_send()
            along_cells(result.at[z], result.at[z], cs_sem.at[z], cr_sem.at[z], sibling).wait_send()

        loop(1, a, ended_z)

    live_here = live[0]
    weights_row = jnp.where(
        lax.broadcasted_iota(jnp.int32, (1, cells), 1) < live_here, 1.0, 0.0
    ).astype(F32)
    weights = jnp.where(
        lax.broadcasted_iota(jnp.int32, (cells, LANES), 0) < live_here, 1.0, 0.0
    ).astype(F32)
    for table in (sl, mr, tl, tr):
        table[...] = jnp.zeros_like(table)
    same = jnp.where(
        lax.broadcasted_iota(jnp.int32, (LANES, LANES), 0)
        == lax.broadcasted_iota(jnp.int32, (LANES, LANES), 1),
        1.0, 0.0,
    ).astype(F32)
    el[...] = same
    er[...] = same
    sl[0:BASIS] = left_basis[...] * weights_row
    gram0[me] = exact_rows(sl[0:BASIS], sl[...])
    spread(along_cells, gram0, me, n, g0s_sem, g0r_sem)

    for _, trio in loads:
        trio[0].wait()
    tiles = width // LANES

    def take_log(d):
        for i in range(tiles):
            here = slice(i * LANES, (i + 1) * LANES)
            values = jnp.log(1.0 + cnt[d, :, here].astype(F32)) * weights
            logged[d, :, here] = values
            w8[d, :, here] = jnp.sum(values.reshape(cells // 8, 8, LANES), axis=0)

    loop(0, n, take_log)
    total_at, total_lane = genes // width, genes % width
    w8[total_at, :, total_lane : total_lane + LANES] = jnp.where(
        lax.broadcasted_iota(jnp.int32, (8, LANES), 0) == 0, live_here.astype(F32), 0.0
    )

    reduce_scatter(lambda d: None, w8, ra8, rt8, rz8, pb8)
    for _, trio in loads:
        trio[1].wait()
        trio[2].wait()

    def fill(d):
        high, low = split(rb[d])
        bhi[d, cells : cells + BASIS + BLOCK] = high
        blo[d, cells : cells + BASIS + BLOCK] = low
        blank = jnp.zeros((LANES - BASIS - BLOCK, width), BF16)
        bhi[d, cells + BASIS + BLOCK :] = blank
        blo[d, cells + BASIS + BLOCK :] = blank

    loop(0, n, fill)
    all_gather(w8, ra8, rt8, rz8, pb8, lambda d: None)
    live_total = jnp.sum(
        pb8[total_at, :, total_lane : total_lane + LANES], axis=0, keepdims=True
    )
    inverse = 1.0 / live_total
    factor_scale = lax.rsqrt(live_total)
    factor_scale = factor_scale * (1.5 - 0.5 * live_total * factor_scale * factor_scale)

    xg0[mine] = jnp.zeros((BASIS + BLOCK, 2 * LANES), F32)

    def center(d):
        for i in range(tiles):
            here = slice(i * LANES, (i + 1) * LANES)
            mean = jnp.sum(pb8[d, :, here], axis=0, keepdims=True) * inverse
            mean = jnp.where(d * width + i * LANES < genes, mean, 0.0)
            high, low = split((logged[d, :, here] - weights * mean) * factor_scale)
            bhi[d, 0:cells, here] = high
            blo[d, 0:cells, here] = low
        high, low = split(rb[d])
        both = jnp.concatenate([high, low], axis=0)
        xg0[mine] = xg0[mine] + product(high, both, bhi[d], blo[d], ROWS)

    loop(0, n, center)
    spread(along_genes, xg0, mine, g, x0s_sem, x0r_sem)
    el[0:BASIS] = gathered(along_cells, gram0, me, n, g0s_sem, g0r_sem)
    el[...] = jnp.where((same > 0) & (lax.broadcasted_iota(jnp.int32, (LANES, LANES), 0) >= BASIS), 1.0, el[...])
    cross = gathered(along_genes, xg0, mine, g, x0s_sem, x0r_sem)
    mr[0 : BASIS + BLOCK] = cross[:, :cells]
    er[0 : BASIS + BLOCK] = cross[:, cells:]
    whole = genes // width

    def update(j):
        later = cells + BASIS + (j + 1) * BLOCK
        later = later if isinstance(j, int) else pl.multiple_of(later, BLOCK)
        chigh, clow = split(chg[...])
        cboth = jnp.concatenate([chigh, clow], axis=0)

        def right(d):
            fresh = product(chigh, cboth, bhi[d, cells:], blo[d, cells:], ALONG)
            vhigh, vlow = split(fresh)
            bhi[d, pl.ds(later, BLOCK)] = vhigh
            blo[d, pl.ds(later, BLOCK)] = vlow
            return fresh * scales[1]

        rows = pl.ds(j * BLOCK if isinstance(j, int) else pl.multiple_of(j * BLOCK, BLOCK), BLOCK)

        def emit(d):
            right_out[rows, pl.ds(pl.multiple_of(d * width, LANES), width)] = right(d)

        loop(0, whole, emit)
        if genes % width:
            right_out[rows, whole * width : genes] = right(whole)[:, : genes % width]

    def step(j):
        position = pl.multiple_of(BASIS + j * BLOCK, BLOCK)
        vectors = mr[pl.ds(position, BLOCK)]
        sl[SLOTS : SLOTS + BLOCK] = vectors
        gram[me] = exact_rows(vectors, sl[...])
        spread(along_cells, gram, me, n, gs_sem, gr_sem)
        pl.when(j > 0)(lambda: update(j - 1))
        total = gathered(along_cells, gram, me, n, gs_sem, gr_sem)
        leftvec, factor, against, _ = orthonormal(total, el[...], tl[...], sl[...], vectors)
        diag_out[j] = factor
        sl[pl.ds(position, BLOCK)] = leftvec
        el[pl.ds(position, BLOCK)] = el[pl.ds(position, BLOCK)] + against
        tl[pl.ds(position, BLOCK)] = against
        left_out[pl.ds(position - BASIS, BLOCK)] = leftvec * scales[0]
        high, low = split(leftvec)
        both = jnp.concatenate([high, low], axis=0)

        def produce(d):
            w[d] = product(high, both, bhi[d, 0:cells], blo[d, 0:cells], ALONG)

        reduce_scatter(produce, w, ra, rt, rz, pb)
        xg[j, mine] = jnp.zeros((BLOCK, 2 * LANES), F32)

        def consume(d):
            phigh, plow = split(pb[d])
            bhi[d, cells + SLOTS : cells + SLOTS + BLOCK] = phigh
            blo[d, cells + SLOTS : cells + SLOTS + BLOCK] = plow
            pboth = jnp.concatenate([phigh, plow], axis=0)
            xg[j, mine] = xg[j, mine] + product(phigh, pboth, bhi[d], blo[d], ROWS)

        all_gather(w, ra, rt, rz, pb, consume)
        box = xg.at[j]
        spread(along_genes, box, mine, g, xs_sem.at[j], xr_sem.at[j])
        total = gathered(along_genes, box, mine, g, xs_sem.at[j], xr_sem.at[j])
        projected, factor, against, change = orthonormal(
            total[:, cells:], er[...], tr[...], mr[...], total[:, :cells]
        )
        couple_out[j] = factor
        later = pl.multiple_of(position + BLOCK, BLOCK)
        mr[pl.ds(later, BLOCK)] = projected
        er[pl.ds(later, BLOCK)] = er[pl.ds(later, BLOCK)] + against
        tr[pl.ds(later, BLOCK)] = against
        chg[...] = change

    loop(0, STEPS, step)
    update(STEPS - 1)


def body(counts, live_rows, left_basis, right_basis, right_start):
    cells, genes = counts.shape
    n = lax.axis_size("cells")
    g = lax.axis_size("genes")
    h = n // 2
    width = -(-(genes // LANES + 1) // n) * LANES
    scales = (math.sqrt(float(cells * n)), math.sqrt(float(genes * g)))
    vmem = pl.BlockSpec(memory_space=pltpu.VMEM)
    anywhere = pl.BlockSpec(memory_space=pl.ANY)
    square = pltpu.VMEM((LANES, LANES), F32)
    dma = lambda *shape: pltpu.SemaphoreType.DMA(shape)
    out_shape = (
        jax.ShapeDtypeStruct((STEPS * BLOCK, cells), F32),
        jax.ShapeDtypeStruct((STEPS * BLOCK, genes), F32),
        jax.ShapeDtypeStruct((STEPS, BLOCK, BLOCK), F32),
        jax.ShapeDtypeStruct((STEPS, BLOCK, BLOCK), F32),
    )
    buffers = lambda rows: [
        pltpu.VMEM((n, rows, width), F32),
        pltpu.VMEM((h, rows, width), F32),
        pltpu.VMEM((h, rows, width), F32),
        pltpu.VMEM((h, rows, width), F32),
        pltpu.VMEM((n, rows, width), F32),
    ]
    scratch = [
        pltpu.VMEM((n, cells, width), jnp.int32),
        pltpu.VMEM((n, cells, width), F32),
        pltpu.VMEM((n, cells + LANES, width), BF16),
        pltpu.VMEM((n, cells + LANES, width), BF16),
        pltpu.VMEM((n, BASIS + BLOCK, width), F32),
        square, square, square, square, square, square,
        *buffers(BLOCK),
        *buffers(8),
        pltpu.VMEM((BLOCK, LANES), F32),
        pltpu.VMEM((n, BASIS, LANES), F32),
        pltpu.VMEM((n, BLOCK, LANES), F32),
        pltpu.VMEM((g, BASIS + BLOCK, 2 * LANES), F32),
        pltpu.VMEM((STEPS, g, BLOCK, 2 * LANES), F32),
        dma(n, 3),
        dma(h), dma(h), dma(h), dma(h), dma(h), dma(n), dma(h), dma(h), dma(h), dma(h),
        dma(n), dma(n), dma(n), dma(n),
        dma(g), dma(g), dma(STEPS, g), dma(STEPS, g),
    ]
    return pl.pallas_call(
        functools.partial(kernel, n, g, width, scales),
        out_shape=out_shape,
        in_specs=[pl.BlockSpec(memory_space=pltpu.SMEM), anywhere, vmem, anywhere, anywhere],
        out_specs=(vmem, vmem, vmem, vmem),
        scratch_shapes=scratch,
        compiler_params=pltpu.CompilerParams(
            collective_id=0, has_side_effects=True, vmem_limit_bytes=66 * 1000 * 1000
        ),
    )(live_rows, counts, left_basis, right_basis, right_start)


def solution(mesh):
    in_specs = (
        P("cells", "genes"),
        P("cells"),
        P(None, "cells"),
        P(None, "genes"),
        P(None, "genes"),
    )
    out_specs = (P(None, "cells"), P(None, "genes"), P(), P())
    return jax.shard_map(body, mesh=mesh, in_specs=in_specs, out_specs=out_specs, check_vma=False)
```

```python
import functools
import math

import jax
import jax.numpy as jnp
from jax import lax
from jax.experimental import pallas as pl
from jax.experimental.pallas import tpu as pltpu
from jax.sharding import PartitionSpec as P

BASIS = 32
BLOCK = 16
STEPS = 3
SLOTS = BASIS + STEPS * BLOCK
LANES = 128
F32 = jnp.float32
BF16 = jnp.bfloat16
HIGHEST = lax.Precision.HIGHEST
MESH = pl.DeviceIdType.MESH


def exact(lhs, rhs):
    return jnp.dot(lhs, rhs, precision=HIGHEST, preferred_element_type=F32)


def exact_rows(lhs, rhs):
    return lax.dot_general(
        lhs, rhs, (((1,), (1,)), ((), ())), precision=HIGHEST, preferred_element_type=F32
    )


def split(values):
    high = values.astype(BF16)
    return high, (values - high.astype(F32)).astype(BF16)


def product(high, both, rhs_high, rhs_low, dims):
    rows = high.shape[0]
    first = lax.dot_general(both, rhs_high, (dims, ((), ())), preferred_element_type=F32)
    second = lax.dot_general(high, rhs_low, (dims, ((), ())), preferred_element_type=F32)
    return first[:rows] + (first[rows:] + second)


ALONG = ((1,), (0,))
ROWS = ((1,), (1,))


def loop(start, stop, step):
    def one(k, carry):
        step(k)
        return carry

    lax.fori_loop(start, stop, one, 0)


def orthonormal(gram, near, lower, spanning, vectors):
    lane = lax.broadcasted_iota(jnp.int32, (BLOCK, LANES), 1)
    row = lax.broadcasted_iota(jnp.int32, (BLOCK, LANES), 0)
    coeffs = jnp.where(lane < SLOTS, gram, 0.0)
    squares = gram[:, SLOTS : SLOTS + BLOCK]
    combined = coeffs + coeffs - (exact(coeffs, near) + exact_rows(coeffs, lower))
    residue = coeffs - (exact(combined, near) + exact_rows(combined, lower))
    squares = squares - exact_rows(combined, coeffs) - exact_rows(residue, combined)
    cleaned = vectors - exact(combined, spanning)
    change = jnp.where(lane == row + SLOTS, 1.0, -combined)
    parts = [squares, cleaned, residue, change]
    for k in range(BLOCK):
        pivot = parts[0][k : k + 1, k : k + 1]
        root = lax.rsqrt(pivot)
        root = root * (1.5 - 0.5 * pivot * root * root)
        column = parts[0][:, k : k + 1] * root
        after = []
        for part in parts:
            scaled = part[k : k + 1, :] * root
            places = lax.broadcasted_iota(jnp.int32, part.shape, 0)
            after.append(
                jnp.where(places > k, part - column * scaled, jnp.where(places == k, scaled, part))
            )
        parts = after
    spot = lax.broadcasted_iota(jnp.int32, (BLOCK, BLOCK), 0)
    other = lax.broadcasted_iota(jnp.int32, (BLOCK, BLOCK), 1)
    upper = jnp.where(other >= spot, parts[0], 0.0)
    factor = exact_rows(jnp.where(other == spot, 1.0, 0.0).astype(F32), upper)
    return parts[1], factor, parts[2], parts[3]


def kernel(
    n, g, width, scales,
    live, counts, left_basis, right_basis, right_start,
    left_out, right_out, diag_out, couple_out,
    cnt, logged, bhi, blo, rb, sl, mr, el, tl, er, tr,
    w, ra, rt, rz, pb, w8, ra8, rt8, rz8, pb8, chg, gram0, gram, xg0, xg,
    in_sem, as_sem, ar_sem, bs_sem, br_sem, cs_sem, cr_sem, ds_sem, fs_sem, zs_sem, zr_sem,
    g0s_sem, g0r_sem, gs_sem, gr_sem, x0s_sem, x0r_sem, xs_sem, xr_sem,
):
    cells, genes = counts.shape
    me = lax.axis_index("cells")
    mine = lax.axis_index("genes")
    core = lax.rem(me, 2)
    chip = me // 2
    h = n // 2
    b = 1 << ((h.bit_length() - 1) // 2)
    b = b if h % b == 0 else 1
    a = h // b
    zi, yi = chip // b, lax.rem(chip, b)
    sibling = me + 1 - 2 * core

    def along_cells(src, dst, send, recv, peer):
        return pltpu.make_async_remote_copy(
            src_ref=src, dst_ref=dst, send_sem=send, recv_sem=recv,
            device_id=(peer, mine), device_id_type=MESH,
        )

    def along_genes(src, dst, send, recv, peer):
        return pltpu.make_async_remote_copy(
            src_ref=src, dst_ref=dst, send_sem=send, recv_sem=recv,
            device_id=(me, peer), device_id_type=MESH,
        )

    loads = []
    for d in range(n):
        cols = max(0, min(width, genes - d * width))
        if cols:
            here = pl.ds(d * width, cols)
            loads.append((d, [
                pltpu.make_async_copy(counts.at[:, here], cnt.at[d, :, pl.ds(0, cols)], in_sem.at[d, 0]),
                pltpu.make_async_copy(right_basis.at[:, here], rb.at[d, pl.ds(0, BASIS), pl.ds(0, cols)], in_sem.at[d, 1]),
                pltpu.make_async_copy(right_start.at[:, here], rb.at[d, pl.ds(BASIS, BLOCK), pl.ds(0, cols)], in_sem.at[d, 2]),
            ]))
        if cols < width:
            cnt[d, :, cols:] = jnp.zeros((cells, width - cols), jnp.int32)
            rb[d, :, cols:] = jnp.zeros((BASIS + BLOCK, width - cols), F32)
    for _, trio in loads:
        trio[0].start()
    for _, trio in loads:
        trio[1].start()
        trio[2].start()

    barrier = pltpu.get_barrier_semaphore()

    def greet_cells(k):
        pl.semaphore_signal(barrier, inc=1, device_id=(lax.rem(me + k, n), mine), device_id_type=MESH)

    def greet_genes(k):
        pl.semaphore_signal(barrier, inc=1, device_id=(me, lax.rem(mine + k, g)), device_id_type=MESH)

    loop(1, n, greet_cells)
    loop(1, g, greet_genes)
    pl.semaphore_wait(barrier, n - 1 + g - 1)

    def spread(copy, buf, at, size, send, recv):
        def go(k):
            copy(buf.at[at], buf.at[at], send.at[k], recv.at[at], lax.rem(at + k, size)).start()

        loop(1, size, go)

    def gathered(copy, buf, at, size, send, recv):
        def end(k):
            source = lax.rem(at + size - k, size)
            item = copy(buf.at[source], buf.at[source], send.at[k], recv.at[source], lax.rem(at + k, size))
            item.wait_send()
            item.wait_recv()

        loop(1, size, end)
        return lax.fori_loop(
            1, size, lambda k, total: total + buf[k], buf[0]
        )

    def order(k):
        return lax.rem(zi + 1 + lax.rem(k, a), a), lax.rem(yi + 1 + k // a, b)

    def reduce_scatter(produce, part, fromcore, fromy, fromz, result):
        def first(k):
            z, y = order(k)
            t = z * b + y
            d = 2 * t + 1 - core
            produce(d)
            along_cells(part.at[d], fromcore.at[t], as_sem.at[t], ar_sem.at[t], sibling).start()

        loop(0, h, first)

        def join(t):
            d = 2 * t + core
            produce(d)
            along_cells(part.at[d], fromcore.at[t], as_sem.at[t], ar_sem.at[t], sibling).wait_recv()
            part[d] = part[d] + fromcore[t]
            return d

        def second(k):
            z, y = order(k)
            t = z * b + y
            d = join(t)
            to = z * b + yi
            along_cells(part.at[d], fromy.at[to], bs_sem.at[t], br_sem.at[to], 2 * (zi * b + y) + core).start()

        loop(0, h - a, second)

        def complete(z):
            d = join(z * b + yi)

            def add(k):
                source = z * b + lax.rem(yi + k, b)
                along_cells(part.at[d], fromy.at[source], bs_sem.at[source], br_sem.at[source], sibling).wait_recv()
                part[d] = part[d] + fromy[source]

            loop(1, b, add)
            return d

        def third(k):
            z = lax.rem(zi + k, a)
            d = complete(z)
            along_cells(part.at[d], fromz.at[zi], zs_sem.at[z], zr_sem.at[zi], d).start()

        loop(1, a, third)
        complete(zi)
        result[me] = part[me]

        def fourth(k):
            z = lax.rem(zi + a - k, a)
            along_cells(part.at[me], fromz.at[z], zs_sem.at[z], zr_sem.at[z], sibling).wait_recv()
            result[me] = result[me] + fromz[z]

        loop(1, a, fourth)

    def all_gather(part, fromcore, fromy, fromz, result, consume):
        def relay(z):
            t = z * b + yi
            d = 2 * t + core

            def to_y(k):
                y = lax.rem(yi + k, b)
                along_cells(result.at[d], result.at[d], fs_sem.at[z * b + y], cr_sem.at[d], 2 * (zi * b + y) + core).start()

            loop(1, b, to_y)
            along_cells(result.at[d], result.at[d], ds_sem.at[t], cr_sem.at[d], sibling).start()

        def arrived(d):
            along_cells(result.at[d], result.at[d], ds_sem.at[0], cr_sem.at[d], sibling).wait_recv()

        def go(k):
            z = lax.rem(zi + k, a)
            along_cells(result.at[me], result.at[me], cs_sem.at[z], cr_sem.at[me], 2 * (z * b + yi) + core).start()

        loop(1, a, go)
        relay(zi)
        consume(me)

        def pass_z(k):
            z = lax.rem(zi + a - k, a)
            d = 2 * (z * b + yi) + core
            arrived(d)
            relay(z)

        loop(1, a, pass_z)
        loop(1, a, lambda k: consume(2 * (lax.rem(zi + a - k, a) * b + yi) + core))

        def pass_y(k):
            z = lax.rem(zi + a - lax.rem(k, a), a)
            t = z * b + lax.rem(yi + 1 + k // a, b)
            d = 2 * t + core
            arrived(d)
            along_cells(result.at[d], result.at[d], ds_sem.at[t], cr_sem.at[d], sibling).start()
            consume(d)

        loop(0, h - a, pass_y)

        def rest(k):
            z = lax.rem(zi + a - lax.rem(k, a), a)
            t = z * b + lax.rem(yi + k // a, b)
            d = 2 * t + 1 - core
            arrived(d)
            consume(d)

        loop(0, h, rest)

        def ended(t):
            along_cells(part.at[t], fromcore.at[t], as_sem.at[t], ar_sem.at[t], sibling).wait_send()
            along_cells(result.at[t], result.at[t], ds_sem.at[t], cr_sem.at[t], sibling).wait_send()

        loop(0, h, ended)

        def ended_y(k):
            z, y = order(k)
            t = z * b + y
            along_cells(part.at[t], fromy.at[t], bs_sem.at[t], br_sem.at[t], sibling).wait_send()
            along_cells(result.at[t], result.at[t], fs_sem.at[t], cr_sem.at[t], sibling).wait_send()

        loop(0, h - a, ended_y)

        def ended_z(k):
            z = lax.rem(zi + k, a)
            along_cells(part.at[z], fromz.at[z], zs_sem.at[z], zr_sem.at[z], sibling).wait_send()
            along_cells(result.at[z], result.at[z], cs_sem.at[z], cr_sem.at[z], sibling).wait_send()

        loop(1, a, ended_z)

    live_here = live[0]
    weights_row = jnp.where(
        lax.broadcasted_iota(jnp.int32, (1, cells), 1) < live_here, 1.0, 0.0
    ).astype(F32)
    weights = jnp.where(
        lax.broadcasted_iota(jnp.int32, (cells, LANES), 0) < live_here, 1.0, 0.0
    ).astype(F32)
    for table in (sl, mr, tl, tr):
        table[...] = jnp.zeros_like(table)
    same = jnp.where(
        lax.broadcasted_iota(jnp.int32, (LANES, LANES), 0)
        == lax.broadcasted_iota(jnp.int32, (LANES, LANES), 1),
        1.0, 0.0,
    ).astype(F32)
    el[...] = same
    er[...] = same
    sl[0:BASIS] = left_basis[...] * weights_row
    gram0[me] = exact_rows(sl[0:BASIS], sl[...])
    spread(along_cells, gram0, me, n, g0s_sem, g0r_sem)

    for _, trio in loads:
        trio[0].wait()
    tiles = width // LANES

    def take_log(d):
        for i in range(tiles):
            here = slice(i * LANES, (i + 1) * LANES)
            values = jnp.log(1.0 + cnt[d, :, here].astype(F32)) * weights
            logged[d, :, here] = values
            w8[d, :, here] = jnp.sum(values.reshape(cells // 8, 8, LANES), axis=0)

    loop(0, n, take_log)
    total_at, total_lane = genes // width, genes % width
    w8[total_at, :, total_lane : total_lane + LANES] = jnp.where(
        lax.broadcasted_iota(jnp.int32, (8, LANES), 0) == 0, live_here.astype(F32), 0.0
    )

    reduce_scatter(lambda d: None, w8, ra8, rt8, rz8, pb8)
    for _, trio in loads:
        trio[1].wait()
        trio[2].wait()

    def fill(d):
        high, low = split(rb[d])
        bhi[d, cells : cells + BASIS + BLOCK] = high
        blo[d, cells : cells + BASIS + BLOCK] = low
        blank = jnp.zeros((LANES - BASIS - BLOCK, width), BF16)
        bhi[d, cells + BASIS + BLOCK :] = blank
        blo[d, cells + BASIS + BLOCK :] = blank

    loop(0, n, fill)
    all_gather(w8, ra8, rt8, rz8, pb8, lambda d: None)
    live_total = jnp.sum(
        pb8[total_at, :, total_lane : total_lane + LANES], axis=0, keepdims=True
    )
    inverse = 1.0 / live_total
    factor_scale = lax.rsqrt(live_total)
    factor_scale = factor_scale * (1.5 - 0.5 * live_total * factor_scale * factor_scale)

    xg0[mine] = jnp.zeros((BASIS + BLOCK, 2 * LANES), F32)

    def center(d):
        for i in range(tiles):
            here = slice(i * LANES, (i + 1) * LANES)
            mean = jnp.sum(pb8[d, :, here], axis=0, keepdims=True) * inverse
            mean = jnp.where(d * width + i * LANES < genes, mean, 0.0)
            high, low = split((logged[d, :, here] - weights * mean) * factor_scale)
            bhi[d, 0:cells, here] = high
            blo[d, 0:cells, here] = low
        high, low = split(rb[d])
        both = jnp.concatenate([high, low], axis=0)
        xg0[mine] = xg0[mine] + product(high, both, bhi[d], blo[d], ROWS)

    loop(0, n, center)
    spread(along_genes, xg0, mine, g, x0s_sem, x0r_sem)
    el[0:BASIS] = gathered(along_cells, gram0, me, n, g0s_sem, g0r_sem)
    el[...] = jnp.where((same > 0) & (lax.broadcasted_iota(jnp.int32, (LANES, LANES), 0) >= BASIS), 1.0, el[...])
    cross = gathered(along_genes, xg0, mine, g, x0s_sem, x0r_sem)
    mr[0 : BASIS + BLOCK] = cross[:, :cells]
    er[0 : BASIS + BLOCK] = cross[:, cells:]
    whole = genes // width

    def update(j):
        later = cells + BASIS + (j + 1) * BLOCK
        later = later if isinstance(j, int) else pl.multiple_of(later, BLOCK)
        chigh, clow = split(chg[...])
        cboth = jnp.concatenate([chigh, clow], axis=0)

        def right(d):
            fresh = product(chigh, cboth, bhi[d, cells:], blo[d, cells:], ALONG)
            vhigh, vlow = split(fresh)
            bhi[d, pl.ds(later, BLOCK)] = vhigh
            blo[d, pl.ds(later, BLOCK)] = vlow
            return fresh * scales[1]

        rows = pl.ds(j * BLOCK if isinstance(j, int) else pl.multiple_of(j * BLOCK, BLOCK), BLOCK)

        def emit(d):
            right_out[rows, pl.ds(pl.multiple_of(d * width, LANES), width)] = right(d)

        loop(0, whole, emit)
        if genes % width:
            right_out[rows, whole * width : genes] = right(whole)[:, : genes % width]

    def step(j):
        position = pl.multiple_of(BASIS + j * BLOCK, BLOCK)
        vectors = mr[pl.ds(position, BLOCK)]
        sl[SLOTS : SLOTS + BLOCK] = vectors
        gram[me] = exact_rows(vectors, sl[...])
        spread(along_cells, gram, me, n, gs_sem, gr_sem)
        pl.when(j > 0)(lambda: update(j - 1))
        total = gathered(along_cells, gram, me, n, gs_sem, gr_sem)
        leftvec, factor, against, _ = orthonormal(total, el[...], tl[...], sl[...], vectors)
        diag_out[j] = factor
        sl[pl.ds(position, BLOCK)] = leftvec
        el[pl.ds(position, BLOCK)] = el[pl.ds(position, BLOCK)] + against
        tl[pl.ds(position, BLOCK)] = against
        left_out[pl.ds(position - BASIS, BLOCK)] = leftvec * scales[0]
        high, low = split(leftvec)
        both = jnp.concatenate([high, low], axis=0)

        def produce(d):
            w[d] = product(high, both, bhi[d, 0:cells], blo[d, 0:cells], ALONG)

        reduce_scatter(produce, w, ra, rt, rz, pb)
        xg[j, mine] = jnp.zeros((BLOCK, 2 * LANES), F32)

        def consume(d):
            phigh, plow = split(pb[d])
            bhi[d, cells + SLOTS : cells + SLOTS + BLOCK] = phigh
            blo[d, cells + SLOTS : cells + SLOTS + BLOCK] = plow
            pboth = jnp.concatenate([phigh, plow], axis=0)
            xg[j, mine] = xg[j, mine] + product(phigh, pboth, bhi[d], blo[d], ROWS)

        all_gather(w, ra, rt, rz, pb, consume)
        box = xg.at[j]
        spread(along_genes, box, mine, g, xs_sem.at[j], xr_sem.at[j])
        total = gathered(along_genes, box, mine, g, xs_sem.at[j], xr_sem.at[j])
        projected, factor, against, change = orthonormal(
            total[:, cells:], er[...], tr[...], mr[...], total[:, :cells]
        )
        couple_out[j] = factor
        later = pl.multiple_of(position + BLOCK, BLOCK)
        mr[pl.ds(later, BLOCK)] = projected
        er[pl.ds(later, BLOCK)] = er[pl.ds(later, BLOCK)] + against
        tr[pl.ds(later, BLOCK)] = against
        chg[...] = change

    loop(0, STEPS, step)
    update(STEPS - 1)


def body(counts, live_rows, left_basis, right_basis, right_start):
    cells, genes = counts.shape
    n = lax.axis_size("cells")
    g = lax.axis_size("genes")
    h = n // 2
    width = -(-(genes // LANES + 1) // n) * LANES
    scales = (math.sqrt(float(cells * n)), math.sqrt(float(genes * g)))
    vmem = pl.BlockSpec(memory_space=pltpu.VMEM)
    anywhere = pl.BlockSpec(memory_space=pl.ANY)
    square = pltpu.VMEM((LANES, LANES), F32)
    dma = lambda *shape: pltpu.SemaphoreType.DMA(shape)
    out_shape = (
        jax.ShapeDtypeStruct((STEPS * BLOCK, cells), F32),
        jax.ShapeDtypeStruct((STEPS * BLOCK, genes), F32),
        jax.ShapeDtypeStruct((STEPS, BLOCK, BLOCK), F32),
        jax.ShapeDtypeStruct((STEPS, BLOCK, BLOCK), F32),
    )
    buffers = lambda rows: [
        pltpu.VMEM((n, rows, width), F32),
        pltpu.VMEM((h, rows, width), F32),
        pltpu.VMEM((h, rows, width), F32),
        pltpu.VMEM((h, rows, width), F32),
        pltpu.VMEM((n, rows, width), F32),
    ]
    scratch = [
        pltpu.VMEM((n, cells, width), jnp.int32),
        pltpu.VMEM((n, cells, width), F32),
        pltpu.VMEM((n, cells + LANES, width), BF16),
        pltpu.VMEM((n, cells + LANES, width), BF16),
        pltpu.VMEM((n, BASIS + BLOCK, width), F32),
        square, square, square, square, square, square,
        *buffers(BLOCK),
        *buffers(8),
        pltpu.VMEM((BLOCK, LANES), F32),
        pltpu.VMEM((n, BASIS, LANES), F32),
        pltpu.VMEM((n, BLOCK, LANES), F32),
        pltpu.VMEM((g, BASIS + BLOCK, 2 * LANES), F32),
        pltpu.VMEM((STEPS, g, BLOCK, 2 * LANES), F32),
        dma(n, 3),
        dma(h), dma(h), dma(h), dma(h), dma(h), dma(n), dma(h), dma(h), dma(h), dma(h),
        dma(n), dma(n), dma(n), dma(n),
        dma(g), dma(g), dma(STEPS, g), dma(STEPS, g),
    ]
    return pl.pallas_call(
        functools.partial(kernel, n, g, width, scales),
        out_shape=out_shape,
        in_specs=[pl.BlockSpec(memory_space=pltpu.SMEM), anywhere, vmem, anywhere, anywhere],
        out_specs=(vmem, vmem, vmem, vmem),
        scratch_shapes=scratch,
        compiler_params=pltpu.CompilerParams(
            collective_id=0, has_side_effects=True, vmem_limit_bytes=66 * 1000 * 1000
        ),
    )(live_rows, counts, left_basis, right_basis, right_start)


def solution(mesh):
    in_specs = (
        P("cells", "genes"),
        P("cells"),
        P(None, "cells"),
        P(None, "genes"),
        P(None, "genes"),
    )
    out_specs = (P(None, "cells"), P(None, "genes"), P(), P())
    return jax.shard_map(body, mesh=mesh, in_specs=in_specs, out_specs=out_specs, check_vma=False)
```
